32 devices in a mesh: dp: 8 (over z, x), seq: 4 (over y, core).
Axes of the slice: x: 2, y: 2, z: 4, core: 2. Of those that a mesh axis runs over, the one named last changes fastest.
Arguments:
- tokens: bfloat16 [24, 1024, 768], P('dp', 'seq'), may hold values from -6 to 6
- lengths: int32 [24], P('dp'), may hold values from 256 to 1024, as said below
- w_qkv: bfloat16 [768, 2304], P(('dp', 'seq')), may hold values from -0.21875 to 0.21875
- w_att_out: bfloat16 [768, 768], P(('dp', 'seq')), may hold values from -1.25 to 1.25
- w_ffin: bfloat16 [768, 4096], P(('dp', 'seq')), may hold values from -0.21875 to 0.21875
- w_ffout: bfloat16 [2048, 768], P(('dp', 'seq')), may hold values from -0.125 to 0.125
- cotangent: bfloat16 [24, 1024, 768], P('dp', 'seq'), may hold values from -6 to 6
Outputs:
- block_output: bfloat16 [24, 1024, 768], P('dp', 'seq')
- grad_tokens: float32 [24, 1024, 768], P('dp', 'seq')
- grad_qkv: float32 [768, 2304], P(('dp', 'seq'))
- grad_att_out: float32 [768, 768], P(('dp', 'seq'))
- grad_ffin: float32 [768, 4096], P(('dp', 'seq'))
- grad_ffout: float32 [2048, 768], P(('dp', 'seq'))
The draws below stay inside these ranges and needn't reach their ends.
Inputs may be any that keep to these rules, and one draw needn't show every extreme that they name: `lengths`: some slot has length exactly 1024 and another exactly 256.
All inputs are finite; a program needn't handle non-finite values.
Results may differ from the reference program's by a relative error of at most 0.014.
Values may be sent and summed in bfloat16 or wider, within the bound.
A program may use at most 192 MiB of HBM per device.

```python
import jax
import jax.numpy as jnp
from jax import lax

D = 768
HEADS = 12
HEAD_DIM = 64
FF = 2048
SLOT = 1024
MIN_LEN = 256
SLOTS = 24


def draw_lengths(key, part):
    base_key, long_key, short_key = jax.random.split(key, 3)
    drawn = jax.random.randint(base_key, (SLOTS,), MIN_LEN, SLOT + 1, dtype=jnp.int32)
    longest = jax.random.randint(long_key, (), 0, SLOTS, dtype=jnp.int32)
    offset = jax.random.randint(short_key, (), 1, SLOTS, dtype=jnp.int32)
    shortest = (longest + offset) % SLOTS
    positions = jnp.arange(SLOTS, dtype=jnp.int32)
    drawn = jnp.where(positions == longest, SLOT, drawn)
    drawn = jnp.where(positions == shortest, MIN_LEN, drawn)
    return drawn.astype(jnp.int32)


def shard_levels(stream_key, extent, pieces, low, top_value):
    level, own = 1.0, jax.random.fold_in(stream_key, 6)
    for dim, parts in pieces:
        draws = jnp.exp(jax.random.uniform(jax.random.fold_in(own, dim), (parts,), jnp.float32, low / len(pieces), top_value / len(pieces)))
        level = level * jnp.repeat(draws, extent[dim] // parts).reshape([-1 if axis == dim else 1 for axis in range(len(extent))])
    return level


def normal_values(stream_key, dims, scale, limit, cuts=(), kind=jnp.bfloat16):
    values = scale * jax.random.normal(stream_key, dims, jnp.float32)
    if cuts:
        values = values * shard_levels(stream_key, dims, cuts, -0.22, 0.18)
    return jnp.clip(values, -limit, limit).astype(kind)


def setup_inputs(seed: int = 0) -> dict:
    seeds = jax.random.split(jax.random.key(seed), 8)
    tokens = normal_values(seeds[0], (SLOTS, SLOT, D), 1.0, 6.0, ((0, 8), (1, 4)))
    lengths = draw_lengths(jax.random.fold_in(seeds[7], 71), 0)
    w_qkv = normal_values(seeds[2], (D, 3 * D), D ** -0.5, 0.21875, ((0, 32),))
    w_att_out = normal_values(seeds[3], (D, D), (D // 32) ** -0.5, 1.25, ((0, 32),))
    w_ffin = normal_values(seeds[4], (D, 2 * FF), D ** -0.5, 0.21875, ((0, 32),))
    w_ffout = normal_values(seeds[5], (FF, D), FF ** -0.5, 0.125, ((0, 32),))
    cotangent = normal_values(seeds[6], (SLOTS, SLOT, D), 1.0, 6.0, ((0, 8), (1, 4)))
    return dict(tokens=tokens, lengths=lengths, w_qkv=w_qkv, w_att_out=w_att_out, w_ffin=w_ffin, w_ffout=w_ffout, cotangent=cotangent)


@jax.custom_vjp
def low(v):
    return lax.optimization_barrier(v.astype(jnp.bfloat16)).astype(jnp.float32)

@jax.custom_vjp
def low_back(v):
    return v

def low_keep(v):
    return (low(v), None)

def low_pass(kept, grad):
    return (grad,)

def back_keep(v):
    return (v, None)

def back_low(kept, grad):
    return (low(grad),)
low.defvjp(low_keep, low_pass)
low_back.defvjp(back_keep, back_low)

def norm_rows(values):
    centred = values - lax.optimization_barrier(jnp.mean(values, axis=-1, keepdims=True))
    spread = lax.optimization_barrier(jnp.mean(centred * centred, axis=-1, keepdims=True))
    return centred * lax.rsqrt(spread + 1e-05)

def rope_tables(positions):
    exponent = jnp.arange(HEAD_DIM // 2, dtype=jnp.float32) * (2.0 / HEAD_DIM)
    frequency = 10000.0 ** (-exponent)
    angles = positions.astype(jnp.float32)[:, None] * frequency[None, :]
    cosine = jnp.concatenate([jnp.cos(angles), jnp.cos(angles)], -1)
    sine_table = jnp.concatenate([jnp.sin(angles), jnp.sin(angles)], -1)
    return (cosine, sine_table)

def rotate(values, cosine, sine_table):
    half_dim = HEAD_DIM // 2
    turned = jnp.concatenate([-values[..., half_dim:], values[..., :half_dim]], -1)
    return values * cosine[:, None, :] + turned * sine_table[:, None, :]

def layer_forward(tokens, w_qkv, w_att_out, w_ffin, w_ffout, length):
    highest = lax.Precision.HIGHEST
    positions = jnp.arange(SLOT, dtype=jnp.int32)
    valid_rows = (positions < length).astype(jnp.float32)[:, None]
    normed = low(norm_rows(tokens))
    project = low_back(jnp.dot(normed, w_qkv, precision=highest)).reshape(SLOT, 3, HEADS, HEAD_DIM)
    cosine, sine_table = rope_tables(positions)
    queries = low(rotate(project[:, 0], cosine, sine_table))
    key_heads = low(rotate(project[:, 1], cosine, sine_table))
    value_heads = low(project[:, 2])
    scores = low_back(jnp.einsum('qhd,khd->hqk', queries, key_heads, precision=highest) * HEAD_DIM ** (-0.5))
    allowed = (positions[None, :] <= positions[:, None]) & (positions[None, :] < length)
    scores = jnp.where(allowed[None], scores, -1e+30)
    weights = low(jax.nn.softmax(scores, axis=-1))
    mixed_heads = jnp.einsum('hqk,khd->qhd', weights, value_heads, precision=highest).reshape(SLOT, HEADS * HEAD_DIM)
    mixed_heads = low_back(low(mixed_heads))
    attended = low_back(jnp.dot(mixed_heads, w_att_out, precision=highest))
    hidden_state = tokens + attended
    normed_two = low(norm_rows(hidden_state))
    gate_up = low_back(jnp.dot(normed_two, w_ffin, precision=highest))
    up_part = gate_up[:, :FF]
    gate_part = gate_up[:, FF:]
    activated = low(jax.nn.silu(gate_part) * up_part)
    branch = low_back(jnp.dot(activated, w_ffout, precision=highest))
    return valid_rows * (hidden_state + branch)

def reference(tokens, lengths, w_qkv, w_att_out, w_ffin, w_ffout, cotangent):
    matrices = (w_qkv.astype(jnp.float32), w_att_out.astype(jnp.float32), w_ffin.astype(jnp.float32), w_ffout.astype(jnp.float32))

    def one_slot(running, slot_item):
        slot_tokens, slot_length, slot_cotangent = slot_item
        result, pull_back = jax.vjp(lambda inputs, first_w, second_w, third_w, fourth_w: layer_forward(inputs, first_w, second_w, third_w, fourth_w, slot_length), slot_tokens.astype(jnp.float32), matrices[0], matrices[1], matrices[2], matrices[3])
        gradients = pull_back(slot_cotangent.astype(jnp.float32))
        running = tuple((total_sum + update for total_sum, update in zip(running, gradients[1:])))
        return (running, (result.astype(jnp.bfloat16), gradients[0]))
    zero_sums = tuple((jnp.zeros_like(matrix) for matrix in matrices))
    running, (outputs, grad_tokens) = lax.scan(one_slot, zero_sums, (tokens, lengths, cotangent))
    return (outputs, grad_tokens, running[0], running[1], running[2], running[3])
```

```python
import functools
import jax
import jax.numpy as jnp
from jax import lax
from jax.experimental import pallas as pl
from jax.experimental.pallas import tpu as pltpu
from jax.sharding import PartitionSpec as P

MESH = pl.DeviceIdType.MESH


def placement():
    dp, seq = lax.axis_index("dp"), lax.axis_index("seq")
    return dp // 2, dp % 2, seq // 2, seq % 2


def device(outer, inner, y, core):
    return {"dp": outer * 2 + inner, "seq": y * 2 + core}


def slot_of(outer, inner, y, core):
    return (outer * 2 + inner) * 4 + y * 2 + core


def greet(n_outer, o, i, y, c):
    barrier = pltpu.get_barrier_semaphore()

    def signal(target):
        pl.semaphore_signal(barrier, inc=1, device_id=target, device_id_type=MESH)

    signal(device(o, 1 - i, y, c))
    signal(device(o, i, 1 - y, c))
    signal(device(o, i, y, 1 - c))

    @pl.when(o > 0)
    def _():
        signal(device(o - 1, i, y, c))

    @pl.when(o < n_outer - 1)
    def _():
        signal(device(o + 1, i, y, c))

    pl.semaphore_wait(barrier, 3 + jnp.where(o > 0, 1, 0) + jnp.where(o < n_outer - 1, 1, 0))


KINDS = ("up", "down", "x", "y", "da", "db", "c_own", "c_x", "c_y", "c_da", "c_db")


class Gather:
    def __init__(self, n_outer, ins, outs, send, recv, local):
        self.n, self.ins, self.outs = n_outer, ins, outs
        self.send_sems, self.recv_sems, self.local = send, recv, local
        self.o, self.i, self.y, self.c = placement()

    def piece(self, a, slot, half=None):
        cols = self.outs[a].shape[2]
        if half is None:
            return self.outs[a].at[slot]
        return self.outs[a].at[slot, :, pl.ds(half * (cols // 2), cols // 2)]

    def copy(self, kind, s, a, src, dst, target):
        k = KINDS.index(kind)
        return pltpu.make_async_remote_copy(
            src_ref=src, dst_ref=dst, send_sem=self.send_sems.at[k, s, a],
            recv_sem=self.recv_sems.at[k, s, a], device_id=target, device_id_type=MESH)

    def arrays(self):
        return range(len(self.ins))

    def send(self, kind, s, slot, target, half=None, own=False):
        for a in self.arrays():
            ref = self.piece(a, slot, half)
            self.copy(kind, s, a, self.ins[a] if own else ref, ref, target).start()

    def wait_recv(self, kind, s, slot, half=None):
        for a in self.arrays():
            ref = self.piece(a, slot, half)
            self.copy(kind, s, a, ref, ref, self.core_mate()).wait_recv()

    def wait_send(self, kind, s, slot, half=None):
        for a in self.arrays():
            ref = self.piece(a, slot, half)
            self.copy(kind, s, a, ref, ref, self.core_mate()).wait_send()

    def x_mate(self):
        return device(self.o, 1 - self.i, self.y, self.c)

    def y_mate(self):
        return device(self.o, self.i, 1 - self.y, self.c)

    def core_mate(self):
        return device(self.o, self.i, self.y, 1 - self.c)

    def spread(self, s, own=False):
        slot = slot_of(s, self.i, self.y, self.c)
        self.send("x", s, slot, self.x_mate(), own=own)
        self.send("y", s, slot, self.y_mate(), own=own)
        self.send("c_own", s, slot, self.core_mate(), own=own)

    def start(self):
        o, i, y, c = self.o, self.i, self.y, self.c
        slot = slot_of(o, i, y, c)

        @pl.when(o < self.n - 1)
        def _():
            self.send("up", o, slot, device(o + 1, i, y, c), own=True)

        @pl.when(o > 0)
        def _():
            self.send("down", o, slot, device(o - 1, i, y, c), own=True)

        self.spread(o, own=True)
        for a in self.arrays():
            pltpu.make_async_copy(self.ins[a], self.piece(a, slot), self.local.at[a]).start()

    def line(self, k):
        o, i, y, c = self.o, self.i, self.y, self.c

        @pl.when(o - k >= 0)
        def _():
            s = o - k
            slot = slot_of(s, i, y, c)
            self.wait_recv("up", s, slot)

            @pl.when(o < self.n - 1)
            def _():
                self.send("up", s, slot, device(o + 1, i, y, c))

            self.spread(s)

        @pl.when(o + k < self.n)
        def _():
            s = o + k
            slot = slot_of(s, i, y, c)
            self.wait_recv("down", s, slot)

            @pl.when(o > 0)
            def _():
                self.send("down", s, slot, device(o - 1, i, y, c))

            self.spread(s)

    def plane(self, s):
        i, y, c = self.i, self.y, self.c
        from_x, from_y = slot_of(s, 1 - i, y, c), slot_of(s, i, 1 - y, c)
        self.wait_recv("x", s, from_x)
        self.send("da", s, from_x, self.y_mate(), half=0)
        self.send("c_x", s, from_x, self.core_mate())
        self.wait_recv("y", s, from_y)
        self.send("db", s, from_y, self.x_mate(), half=1)
        self.send("c_y", s, from_y, self.core_mate())

    def far(self, s):
        i, y, c = self.i, self.y, self.c
        slot = slot_of(s, 1 - i, 1 - y, c)
        self.wait_recv("da", s, slot, half=0)
        self.send("c_da", s, slot, self.core_mate(), half=0)
        self.wait_recv("db", s, slot, half=1)
        self.send("c_db", s, slot, self.core_mate(), half=1)

    def both(self, k, step):
        if k == 0:
            step(self.o)
            return

        @pl.when(self.o - k >= 0)
        def _():
            step(self.o - k)

        @pl.when(self.o + k < self.n)
        def _():
            step(self.o + k)

    def finish(self):
        o, i, y, c = self.o, self.i, self.y, self.c

        def close(s, carry):
            other = 1 - c
            self.wait_recv("c_own", s, slot_of(s, i, y, other))
            self.wait_recv("c_x", s, slot_of(s, 1 - i, y, other))
            self.wait_recv("c_y", s, slot_of(s, i, 1 - y, other))
            self.wait_recv("c_da", s, slot_of(s, 1 - i, 1 - y, other), half=0)
            self.wait_recv("c_db", s, slot_of(s, 1 - i, 1 - y, other), half=1)
            slot = slot_of(s, i, y, c)
            for kind in ("x", "y", "c_own", "c_x", "c_y"):
                self.wait_send(kind, s, slot)
            self.wait_send("da", s, slot, half=0)
            self.wait_send("db", s, slot, half=1)
            self.wait_send("c_da", s, slot, half=0)
            self.wait_send("c_db", s, slot, half=1)

            @pl.when((s <= o) & (o < self.n - 1))
            def _():
                self.wait_send("up", s, slot)

            @pl.when((s >= o) & (o > 0))
            def _():
                self.wait_send("down", s, slot)

            return carry

        lax.fori_loop(0, self.n, close, 0)
        for a in self.arrays():
            pltpu.make_async_copy(self.ins[a], self.piece(a, slot_of(o, i, y, c)), self.local.at[a]).wait()

    def stages(self):
        todo = [lambda: self.start()]
        for k in range(self.n):
            if k + 1 < self.n:
                todo.append(functools.partial(self.line, k + 1))
            todo.append(functools.partial(self.both, k, self.plane))
            todo.append(functools.partial(self.both, k, self.far))
        todo.append(self.finish)
        return todo


def gather_scratch(n_outer, count):
    return [
        pltpu.SemaphoreType.DMA((len(KINDS), n_outer, count)),
        pltpu.SemaphoreType.DMA((len(KINDS), n_outer, count)),
        pltpu.SemaphoreType.DMA((count,)),
    ]


def gather_rows(shards, collective_id):
    n_outer = lax.axis_size("dp") // 2
    count = len(shards)

    def kernel(*refs):
        ins, outs = refs[:count], refs[count:2 * count]
        send, recv, local = refs[2 * count:]
        greet(n_outer, *placement())
        for stage in Gather(n_outer, ins, outs, send, recv, local).stages():
            stage()

    devices = lax.axis_size(("dp", "seq"))
    return pl.pallas_call(
        kernel,
        out_shape=[jax.ShapeDtypeStruct((devices,) + v.shape, v.dtype) for v in shards],
        in_specs=[pl.BlockSpec(memory_space=pl.ANY)] * count,
        out_specs=[pl.BlockSpec(memory_space=pl.ANY)] * count,
        scratch_shapes=gather_scratch(n_outer, count),
        compiler_params=pltpu.CompilerParams(collective_id=collective_id, has_side_effects=True),
        name="gather_rows",
    )(*shards)

HEAD_DIM = 64

RKINDS = ("da", "db", "x", "y", "up", "down")


class Scatter:
    def __init__(self, n_outer, ins, outs, scratch):
        count = len(ins)
        self.n, self.ins, self.outs, self.count = n_outer, ins, outs, count
        groups = [scratch[g * count:(g + 1) * count] for g in range(7)]
        self.acc, self.cbuf, self.far, self.xbuf, self.ybuf, self.upbuf, self.downbuf = groups
        self.send_sems, self.recv_sems, self.local = scratch[7 * count:]
        self.o, self.i, self.y, self.c = placement()

    def half(self, ref, h):
        cols = ref.shape[-1] // 2
        return ref.at[:, pl.ds(h * cols, cols)]

    def quad(self, i, y):
        return i * 2 + y

    def core_copy(self, s, a, q):
        slot = slot_of(s, q // 2, q % 2, 1 - self.c)
        return pltpu.make_async_remote_copy(
            src_ref=self.ins[a].at[slot], dst_ref=self.cbuf[a].at[s, q],
            send_sem=self.send_sems.at[len(RKINDS) + q, s, a], recv_sem=self.recv_sems.at[len(RKINDS) + q, s, a],
            device_id=device(self.o, self.i, self.y, 1 - self.c), device_id_type=MESH)

    def own_copy(self, s, a, q):
        slot = slot_of(s, q // 2, q % 2, self.c)
        return pltpu.make_async_copy(self.ins[a].at[slot], self.acc[a].at[s, q], self.local.at[s, a, q])

    def hop(self, kind, s, a):
        o, i, y, c = self.o, self.i, self.y, self.c
        far, via_x, via_y, own = (self.quad(1 - i, 1 - y), self.quad(1 - i, y), self.quad(i, 1 - y), self.quad(i, y))
        acc = self.acc[a]
        plan = {
            "da": lambda: (self.half(acc.at[s, far], 0), self.far[a].at[0, s], device(o, i, 1 - y, c)),
            "db": lambda: (self.half(acc.at[s, far], 1), self.far[a].at[1, s], device(o, 1 - i, y, c)),
            "x": lambda: (acc.at[s, via_x], self.xbuf[a].at[s], device(o, 1 - i, y, c)),
            "y": lambda: (acc.at[s, via_y], self.ybuf[a].at[s], device(o, i, 1 - y, c)),
            "up": lambda: (acc.at[s, own], self.upbuf[a].at[s], device(o + 1, i, y, c)),
            "down": lambda: (acc.at[s, own], self.downbuf[a].at[s], device(o - 1, i, y, c)),
        }
        src, dst, target = plan[kind]()
        k = RKINDS.index(kind)
        return pltpu.make_async_remote_copy(
            src_ref=src, dst_ref=dst, send_sem=self.send_sems.at[k, s, a],
            recv_sem=self.recv_sems.at[k, s, a], device_id=target, device_id_type=MESH)

    def target_slice(self, t):
        return jnp.where(t % 2 == 0, self.n - 1 - t // 2, t // 2)

    def begin(self, t, carry):
        s = self.target_slice(t)
        for a in range(self.count):
            for j in range(4):
                q = 3 - j
                self.core_copy(s, a, q).start()
                self.own_copy(s, a, q).start()
        return carry

    def pair(self, s, a):
        for q in range(4):
            self.core_copy(s, a, q).wait_recv()
            self.own_copy(s, a, q).wait()
            self.acc[a][s, q] = (self.acc[a][s, q].astype(jnp.float32)
                                 + self.cbuf[a][s, q].astype(jnp.float32)).astype(jnp.bfloat16)

    def first(self, s):
        for a in range(self.count):
            self.pair(s, a)
            self.hop("da", s, a).start()
            self.hop("db", s, a).start()

    def second(self, s):
        for a in range(self.count):
            cols = self.acc[a].shape[-1] // 2
            for h, kind, q in ((0, "da", self.quad(1 - self.i, self.y)), (1, "db", self.quad(self.i, 1 - self.y))):
                self.hop(kind, s, a).wait_recv()
                window = pl.ds(h * cols, cols)
                self.acc[a][s, q, :, window] = (
                    self.acc[a][s, q, :, window].astype(jnp.float32)
                    + self.far[a][h, s].astype(jnp.float32)).astype(jnp.bfloat16)
                self.hop("x" if h == 0 else "y", s, a).start()

    def third(self, s):
        o, q = self.o, self.quad(self.i, self.y)
        for a in range(self.count):
            self.hop("x", s, a).wait_recv()
            self.hop("y", s, a).wait_recv()
            total = (self.acc[a][s, q].astype(jnp.float32) + self.xbuf[a][s].astype(jnp.float32)
                     + self.ybuf[a][s].astype(jnp.float32))

            @pl.when(s != o)
            def _():
                self.acc[a][s, q] = total.astype(jnp.bfloat16)

            @pl.when(s == o)
            def _():
                self.outs[a][...] = total

        for a in range(self.count):
            for kind, ahead, has_before, buf in (
                ("up", s > o, o > 0, self.upbuf), ("down", s < o, o < self.n - 1, self.downbuf)):

                @pl.when(ahead)
                def _(kind=kind, has_before=has_before, buf=buf, a=a):
                    @pl.when(has_before)
                    def _():
                        self.hop(kind, s, a).wait_recv()
                        self.acc[a][s, q] = (self.acc[a][s, q].astype(jnp.float32)
                                             + buf[a][s].astype(jnp.float32)).astype(jnp.bfloat16)

                    self.hop(kind, s, a).start()

    def step(self, t, carry):
        n = self.n

        @pl.when(t < n)
        def _():
            self.first(self.target_slice(t))

        @pl.when((t >= 1) & (t < n + 1))
        def _():
            self.second(self.target_slice(t - 1))

        @pl.when(t >= 2)
        def _():
            self.third(self.target_slice(t - 2))

        return carry

    def finish(self):
        o = self.o
        for a in range(self.count):
            for kind, there, buf in (("up", o > 0, self.upbuf), ("down", o < self.n - 1, self.downbuf)):

                @pl.when(there)
                def _(kind=kind, buf=buf, a=a):
                    self.hop(kind, o, a).wait_recv()
                    self.outs[a][...] += buf[a][o].astype(jnp.float32)

        def close(s, carry):
            for a in range(self.count):
                for q in range(4):
                    self.core_copy(s, a, q).wait_send()
                for kind in ("da", "db", "x", "y"):
                    self.hop(kind, s, a).wait_send()

                @pl.when(s > o)
                def _(a=a):
                    self.hop("up", s, a).wait_send()

                @pl.when(s < o)
                def _(a=a):
                    self.hop("down", s, a).wait_send()

            return carry

        lax.fori_loop(0, self.n, close, 0)

    def run(self):
        lax.fori_loop(0, self.n, self.begin, 0)
        lax.fori_loop(0, self.n + 2, self.step, 0)
        self.finish()


def scatter_scratch(n, shapes):
    bf = jnp.bfloat16
    scratch = [pltpu.VMEM((n, 4) + s, bf) for s in shapes]
    scratch += [pltpu.VMEM((n, 4) + s, bf) for s in shapes]
    scratch += [pltpu.VMEM((2, n, s[0], s[1] // 2), bf) for s in shapes]
    for _ in range(4):
        scratch += [pltpu.VMEM((n,) + s, bf) for s in shapes]
    count = len(shapes)
    scratch += [pltpu.SemaphoreType.DMA((len(RKINDS) + 4, n, count)) for _ in range(2)]
    scratch += [pltpu.SemaphoreType.DMA((n, count, 4))]
    return scratch


def scatter_rows(blocks, collective_id):
    n_outer = lax.axis_size("dp") // 2
    count = len(blocks)
    shapes = [b.shape[1:] for b in blocks]

    def kernel(*refs):
        ins, outs, scratch = refs[:count], refs[count:2 * count], refs[2 * count:]
        work = Scatter(n_outer, ins, outs, scratch)
        greet(n_outer, *placement())
        work.run()

    return pl.pallas_call(
        kernel,
        out_shape=[jax.ShapeDtypeStruct(s, jnp.float32) for s in shapes],
        in_specs=[pl.BlockSpec(memory_space=pl.ANY)] * count,
        out_specs=[pl.BlockSpec(memory_space=pltpu.VMEM)] * count,
        scratch_shapes=scatter_scratch(n_outer, shapes),
        compiler_params=pltpu.CompilerParams(collective_id=collective_id, has_side_effects=True, vmem_limit_bytes=56 << 20),
        name="scatter_rows",
    )(*blocks)


def norm_rows(values):
    centred = values - jnp.mean(values, axis=-1, keepdims=True)
    spread = jnp.mean(centred * centred, axis=-1, keepdims=True)
    inverse = lax.rsqrt(spread + 1e-05)
    return (centred * inverse, inverse)


def norm_back(grad_in, normed, inverse):
    mean_grad = jnp.mean(grad_in, axis=-1, keepdims=True)
    mean_prod = jnp.mean(grad_in * normed, axis=-1, keepdims=True)
    return (grad_in - mean_grad - normed * mean_prod) * inverse


def rope_tables(positions):
    exponent = jnp.arange(HEAD_DIM // 2, dtype=jnp.float32) * (2.0 / HEAD_DIM)
    frequency = 10000.0 ** (-exponent)
    angles = positions.astype(jnp.float32)[:, None] * frequency[None, :]
    cosine = jnp.concatenate([jnp.cos(angles), jnp.cos(angles)], -1)
    sine_table = jnp.concatenate([jnp.sin(angles), jnp.sin(angles)], -1)
    return (cosine[None, :, None, :], sine_table[None, :, None, :])


def rotate(values, cosine, sine_table):
    half_dim = values.shape[-1] // 2
    turned = jnp.concatenate([-values[..., half_dim:], values[..., :half_dim]], -1)
    return values * cosine + turned * sine_table


def rotate_back(grad_in, cosine, sine_table):
    half_dim = grad_in.shape[-1] // 2
    scaled = grad_in * sine_table
    return grad_in * cosine + jnp.concatenate([scaled[..., half_dim:], -scaled[..., :half_dim]], -1)


def contract_last(left_side, right_side):
    return lax.dot_general(
        left_side, right_side, (((1,), (1,)), ((), ())), preferred_element_type=jnp.float32
    )


def gather_weights(first, second, collective_id):
    one, two = gather_rows((first, second), collective_id)
    return one.reshape(-1, first.shape[1]), two.reshape(-1, second.shape[1])


def weight_term(left_side, right_side):
    term = lax.dot_general(
        left_side, right_side, (((0,), (0,)), ((), ())), preferred_element_type=jnp.float32
    )
    return term.astype(jnp.bfloat16).reshape(lax.axis_size(("dp", "seq")), -1, term.shape[1])


def on_device(tokens, lengths, w_qkv, w_att_out, w_ffin, w_ffout, cotangent):
    slot_count, local_len, model_width = tokens.shape
    head_count = model_width // HEAD_DIM
    row_count = slot_count * local_len
    slot_len = local_len * lax.axis_size("seq")
    positions = lax.axis_index("seq") * local_len + jnp.arange(local_len, dtype=jnp.int32)
    key_positions = jnp.arange(slot_len, dtype=jnp.int32)
    valid_rows = (positions[None, :] < lengths[:, None]).astype(jnp.float32)[:, :, None]
    cosine, sine_table = rope_tables(positions)
    score_scale = HEAD_DIM ** (-0.5)

    def masked_scores(query_one, key_one, length):
        allowed = (key_positions[None, :] <= positions[:, None]) & (key_positions[None, :] < length)
        raw_scores = (
            jnp.einsum("qhd,khd->hqk", query_one, key_one, preferred_element_type=jnp.float32)
            * score_scale
        )
        return jnp.where(allowed[None], raw_scores, -1e30)

    def forward_slot(item):
        query_one, key_one, value_one, length = item
        scores = masked_scores(query_one, key_one, length)
        row_top = jnp.max(scores, axis=-1, keepdims=True)
        exponent_terms = jnp.exp(scores - row_top)
        row_total = jnp.sum(exponent_terms, axis=-1, keepdims=True)
        probs_bf = (exponent_terms / row_total).astype(jnp.bfloat16)
        mixed_one = jnp.einsum(
            "hqk,khd->qhd", probs_bf, value_one, preferred_element_type=jnp.float32
        )
        return (mixed_one.astype(jnp.bfloat16), row_top + jnp.log(row_total))

    def backward_slot(item):
        query_one, key_one, value_one, grad_mixed_one, log_one, length = item
        probs_again = jnp.exp(masked_scores(query_one, key_one, length) - log_one)
        probs_again_bf = probs_again.astype(jnp.bfloat16)
        grad_probs = jnp.einsum(
            "qhd,khd->hqk", grad_mixed_one, value_one, preferred_element_type=jnp.float32
        )
        grad_scores = probs_again * (
            grad_probs - jnp.sum(probs_again * grad_probs, axis=-1, keepdims=True)
        )
        grad_scores_bf = grad_scores.astype(jnp.bfloat16)
        grad_query_one = (
            jnp.einsum("hqk,khd->qhd", grad_scores_bf, key_one, preferred_element_type=jnp.float32)
            * score_scale
        )
        grad_key_one = (
            jnp.einsum(
                "hqk,qhd->khd", grad_scores_bf, query_one, preferred_element_type=jnp.float32
            )
            * score_scale
        )
        grad_value_one = jnp.einsum(
            "hqk,qhd->khd", probs_again_bf, grad_mixed_one, preferred_element_type=jnp.float32
        )
        return (grad_query_one, grad_key_one, grad_value_one)

    inputs = tokens.astype(jnp.float32).reshape(row_count, model_width)
    normed_one, inverse_one = norm_rows(inputs)
    normed_one_bf = normed_one.astype(jnp.bfloat16)
    qkv_full, att_out_full = gather_weights(w_qkv, w_att_out, 1)
    project = jnp.dot(normed_one_bf, qkv_full, preferred_element_type=jnp.float32)
    project = project.reshape(slot_count, local_len, 3, head_count, HEAD_DIM)
    query_bf = rotate(project[:, :, 0], cosine, sine_table).astype(jnp.bfloat16)
    key_bf = rotate(project[:, :, 1], cosine, sine_table).astype(jnp.bfloat16)
    value_bf = project[:, :, 2].astype(jnp.bfloat16)
    key_all, value_all = (
        lax.all_gather(key_bf, "seq", axis=1, tiled=True),
        lax.all_gather(value_bf, "seq", axis=1, tiled=True),
    )
    mixed_slots, log_total = lax.map(forward_slot, (query_bf, key_all, value_all, lengths))
    mixed_bf = mixed_slots.reshape(row_count, model_width)
    hidden_state = inputs + jnp.dot(mixed_bf, att_out_full, preferred_element_type=jnp.float32)
    normed_two, inverse_two = norm_rows(hidden_state)
    normed_two_bf = normed_two.astype(jnp.bfloat16)
    ffin_full, ffout_full = gather_weights(w_ffin, w_ffout, 2)
    gate_up = jnp.dot(normed_two_bf, ffin_full, preferred_element_type=jnp.float32)
    half_units = gate_up.shape[1] // 2
    up_part = gate_up[:, :half_units]
    gate_part = gate_up[:, half_units:]
    gate_sigmoid = jax.nn.sigmoid(gate_part)
    activated_bf = (gate_part * gate_sigmoid * up_part).astype(jnp.bfloat16)
    branch = jnp.dot(activated_bf, ffout_full, preferred_element_type=jnp.float32)
    block_output = (valid_rows * (hidden_state + branch).reshape(tokens.shape)).astype(jnp.bfloat16)
    grad_out = (valid_rows * cotangent.astype(jnp.float32)).reshape(row_count, model_width)
    grad_out_bf = grad_out.astype(jnp.bfloat16)
    ffin_back, ffout_back = ffin_full, ffout_full
    grad_act = contract_last(grad_out_bf, ffout_back)
    grad_up = grad_act * gate_part * gate_sigmoid
    grad_gate = grad_act * up_part * gate_sigmoid * (1.0 + gate_part * (1.0 - gate_sigmoid))
    grad_gate_up_bf = jnp.concatenate([grad_up, grad_gate], 1).astype(jnp.bfloat16)
    grad_normed_two = contract_last(grad_gate_up_bf, ffin_back)
    grad_hidden = grad_out + norm_back(grad_normed_two, normed_two, inverse_two)
    grad_hidden_bf = grad_hidden.astype(jnp.bfloat16)
    qkv_back, att_out_back = qkv_full, att_out_full
    grad_mixed_bf = contract_last(grad_hidden_bf, att_out_back).astype(jnp.bfloat16)
    grad_mixed_bf = grad_mixed_bf.reshape(slot_count, local_len, head_count, HEAD_DIM)
    key_use, value_use = (key_all, value_all)
    grad_query, grad_key_all, grad_value_all = lax.map(
        backward_slot, (query_bf, key_use, value_use, grad_mixed_bf, log_total, lengths)
    )
    grad_key, grad_value = (
        lax.psum_scatter(
            grad_key_all.astype(jnp.bfloat16), "seq", scatter_dimension=1, tiled=True
        ).astype(jnp.float32),
        lax.psum_scatter(
            grad_value_all.astype(jnp.bfloat16), "seq", scatter_dimension=1, tiled=True
        ).astype(jnp.float32),
    )
    grad_project_bf = jnp.stack(
        [
            rotate_back(grad_query, cosine, sine_table),
            rotate_back(grad_key, cosine, sine_table),
            grad_value,
        ],
        2,
    )
    grad_project_bf = grad_project_bf.reshape(row_count, 3 * model_width).astype(jnp.bfloat16)
    grad_normed_one = contract_last(grad_project_bf, qkv_back)
    grad_tokens = grad_hidden + norm_back(grad_normed_one, normed_one, inverse_one)
    grad_qkv, grad_att_out, grad_ffin, grad_ffout = scatter_rows(
        (
            weight_term(normed_one_bf, grad_project_bf),
            weight_term(mixed_bf, grad_hidden_bf),
            weight_term(normed_two_bf, grad_gate_up_bf),
            weight_term(activated_bf, grad_out_bf),
        ),
        3,
    )
    return (
        block_output,
        grad_tokens.reshape(tokens.shape),
        grad_qkv,
        grad_att_out,
        grad_ffin,
        grad_ffout,
    )


def solution(mesh):
    placed = (
        P("dp", "seq", None),
        P("dp"),
        P(("dp", "seq"), None),
        P(("dp", "seq"), None),
        P(("dp", "seq"), None),
        P(("dp", "seq"), None),
        P("dp", "seq", None),
    )
    return jax.shard_map(
        on_device,
        mesh=mesh,
        in_specs=placed,
        out_specs=(
            P("dp", "seq", None),
            P("dp", "seq", None),
            P(("dp", "seq"), None),
            P(("dp", "seq"), None),
            P(("dp", "seq"), None),
            P(("dp", "seq"), None),
        ),
        check_vma=False,
    )
```

```python
import functools
import jax
import jax.numpy as jnp
from jax import lax
from jax.experimental import pallas as pl
from jax.experimental.pallas import tpu as pltpu
from jax.sharding import PartitionSpec as P

MESH = pl.DeviceIdType.MESH


def placement():
    dp, seq = lax.axis_index("dp"), lax.axis_index("seq")
    return dp // 2, dp % 2, seq // 2, seq % 2


def device(outer, inner, y, core):
    return {"dp": outer * 2 + inner, "seq": y * 2 + core}


def slot_of(outer, inner, y, core):
    return (outer * 2 + inner) * 4 + y * 2 + core


def greet(n_outer, o, i, y, c):
    barrier = pltpu.get_barrier_semaphore()

    def signal(target):
        pl.semaphore_signal(barrier, inc=1, device_id=target, device_id_type=MESH)

    signal(device(o, 1 - i, y, c))
    signal(device(o, i, 1 - y, c))
    signal(device(o, i, y, 1 - c))

    @pl.when(o > 0)
    def _():
        signal(device(o - 1, i, y, c))

    @pl.when(o < n_outer - 1)
    def _():
        signal(device(o + 1, i, y, c))

    pl.semaphore_wait(barrier, 3 + jnp.where(o > 0, 1, 0) + jnp.where(o < n_outer - 1, 1, 0))


KINDS = ("up", "down", "x", "y", "da", "db", "c_own", "c_x", "c_y", "c_da", "c_db")


class Gather:
    def __init__(self, n_outer, ins, outs, send, recv, local):
        self.n, self.ins, self.outs = n_outer, ins, outs
        self.send_sems, self.recv_sems, self.local = send, recv, local
        self.o, self.i, self.y, self.c = placement()

    def piece(self, a, slot, half=None):
        cols = self.outs[a].shape[2]
        if half is None:
            return self.outs[a].at[slot]
        return self.outs[a].at[slot, :, pl.ds(half * (cols // 2), cols // 2)]

    def copy(self, kind, s, a, src, dst, target):
        k = KINDS.index(kind)
        return pltpu.make_async_remote_copy(
            src_ref=src, dst_ref=dst, send_sem=self.send_sems.at[k, s, a],
            recv_sem=self.recv_sems.at[k, s, a], device_id=target, device_id_type=MESH)

    def arrays(self):
        return range(len(self.ins))

    def send(self, kind, s, slot, target, half=None, own=False):
        for a in self.arrays():
            ref = self.piece(a, slot, half)
            self.copy(kind, s, a, self.ins[a] if own else ref, ref, target).start()

    def wait_recv(self, kind, s, slot, half=None):
        for a in self.arrays():
            ref = self.piece(a, slot, half)
            self.copy(kind, s, a, ref, ref, self.core_mate()).wait_recv()

    def wait_send(self, kind, s, slot, half=None):
        for a in self.arrays():
            ref = self.piece(a, slot, half)
            self.copy(kind, s, a, ref, ref, self.core_mate()).wait_send()

    def x_mate(self):
        return device(self.o, 1 - self.i, self.y, self.c)

    def y_mate(self):
        return device(self.o, self.i, 1 - self.y, self.c)

    def core_mate(self):
        return device(self.o, self.i, self.y, 1 - self.c)

    def spread(self, s, own=False):
        slot = slot_of(s, self.i, self.y, self.c)
        self.send("x", s, slot, self.x_mate(), own=own)
        self.send("y", s, slot, self.y_mate(), own=own)
        self.send("c_own", s, slot, self.core_mate(), own=own)

    def start(self):
        o, i, y, c = self.o, self.i, self.y, self.c
        slot = slot_of(o, i, y, c)

        @pl.when(o < self.n - 1)
        def _():
            self.send("up", o, slot, device(o + 1, i, y, c), own=True)

        @pl.when(o > 0)
        def _():
            self.send("down", o, slot, device(o - 1, i, y, c), own=True)

        self.spread(o, own=True)
        for a in self.arrays():
            pltpu.make_async_copy(self.ins[a], self.piece(a, slot), self.local.at[a]).start()

    def line(self, k):
        o, i, y, c = self.o, self.i, self.y, self.c

        @pl.when(o - k >= 0)
        def _():
            s = o - k
            slot = slot_of(s, i, y, c)
            self.wait_recv("up", s, slot)

            @pl.when(o < self.n - 1)
            def _():
                self.send("up", s, slot, device(o + 1, i, y, c))

            self.spread(s)

        @pl.when(o + k < self.n)
        def _():
            s = o + k
            slot = slot_of(s, i, y, c)
            self.wait_recv("down", s, slot)

            @pl.when(o > 0)
            def _():
                self.send("down", s, slot, device(o - 1, i, y, c))

            self.spread(s)

    def plane(self, s):
        i, y, c = self.i, self.y, self.c
        from_x, from_y = slot_of(s, 1 - i, y, c), slot_of(s, i, 1 - y, c)
        self.wait_recv("x", s, from_x)
        self.send("da", s, from_x, self.y_mate(), half=0)
        self.send("c_x", s, from_x, self.core_mate())
        self.wait_recv("y", s, from_y)
        self.send("db", s, from_y, self.x_mate(), half=1)
        self.send("c_y", s, from_y, self.core_mate())

    def far(self, s):
        i, y, c = self.i, self.y, self.c
        slot = slot_of(s, 1 - i, 1 - y, c)
        self.wait_recv("da", s, slot, half=0)
        self.send("c_da", s, slot, self.core_mate(), half=0)
        self.wait_recv("db", s, slot, half=1)
        self.send("c_db", s, slot, self.core_mate(), half=1)

    def both(self, k, step):
        if k == 0:
            step(self.o)
            return

        @pl.when(self.o - k >= 0)
        def _():
            step(self.o - k)

        @pl.when(self.o + k < self.n)
        def _():
            step(self.o + k)

    def finish(self):
        o, i, y, c = self.o, self.i, self.y, self.c

        def close(s, carry):
            other = 1 - c
            self.wait_recv("c_own", s, slot_of(s, i, y, other))
            self.wait_recv("c_x", s, slot_of(s, 1 - i, y, other))
            self.wait_recv("c_y", s, slot_of(s, i, 1 - y, other))
            self.wait_recv("c_da", s, slot_of(s, 1 - i, 1 - y, other), half=0)
            self.wait_recv("c_db", s, slot_of(s, 1 - i, 1 - y, other), half=1)
            slot = slot_of(s, i, y, c)
            for kind in ("x", "y", "c_own", "c_x", "c_y"):
                self.wait_send(kind, s, slot)
            self.wait_send("da", s, slot, half=0)
            self.wait_send("db", s, slot, half=1)
            self.wait_send("c_da", s, slot, half=0)
            self.wait_send("c_db", s, slot, half=1)

            @pl.when((s <= o) & (o < self.n - 1))
            def _():
                self.wait_send("up", s, slot)

            @pl.when((s >= o) & (o > 0))
            def _():
                self.wait_send("down", s, slot)

            return carry

        lax.fori_loop(0, self.n, close, 0)
        for a in self.arrays():
            pltpu.make_async_copy(self.ins[a], self.piece(a, slot_of(o, i, y, c)), self.local.at[a]).wait()

    def stages(self):
        todo = [lambda: self.start()]
        for k in range(self.n):
            if k + 1 < self.n:
                todo.append(functools.partial(self.line, k + 1))
            todo.append(functools.partial(self.both, k, self.plane))
            todo.append(functools.partial(self.both, k, self.far))
        todo.append(self.finish)
        return todo


def gather_scratch(n_outer, count):
    return [
        pltpu.SemaphoreType.DMA((len(KINDS), n_outer, count)),
        pltpu.SemaphoreType.DMA((len(KINDS), n_outer, count)),
        pltpu.SemaphoreType.DMA((count,)),
    ]


def gather_rows(shards, collective_id):
    n_outer = lax.axis_size("dp") // 2
    count = len(shards)

    def kernel(*refs):
        ins, outs = refs[:count], refs[count:2 * count]
        send, recv, local = refs[2 * count:]
        greet(n_outer, *placement())
        for stage in Gather(n_outer, ins, outs, send, recv, local).stages():
            stage()

    devices = lax.axis_size(("dp", "seq"))
    return pl.pallas_call(
        kernel,
        out_shape=[jax.ShapeDtypeStruct((devices,) + v.shape, v.dtype) for v in shards],
        in_specs=[pl.BlockSpec(memory_space=pl.ANY)] * count,
        out_specs=[pl.BlockSpec(memory_space=pl.ANY)] * count,
        scratch_shapes=gather_scratch(n_outer, count),
        compiler_params=pltpu.CompilerParams(collective_id=collective_id, has_side_effects=True),
        name="gather_rows",
    )(*shards)

HEAD_DIM = 64

RKINDS = ("da", "db", "x", "y", "up", "down")


class Scatter:
    def __init__(self, n_outer, ins, outs, scratch):
        count = len(ins)
        self.n, self.ins, self.outs, self.count = n_outer, ins, outs, count
        groups = [scratch[g * count:(g + 1) * count] for g in range(7)]
        self.acc, self.cbuf, self.far, self.xbuf, self.ybuf, self.upbuf, self.downbuf = groups
        self.send_sems, self.recv_sems, self.local = scratch[7 * count:]
        self.o, self.i, self.y, self.c = placement()

    def half(self, ref, h):
        cols = ref.shape[-1] // 2
        return ref.at[:, pl.ds(h * cols, cols)]

    def quad(self, i, y):
        return i * 2 + y

    def core_copy(self, s, a, q):
        slot = slot_of(s, q // 2, q % 2, 1 - self.c)
        return pltpu.make_async_remote_copy(
            src_ref=self.ins[a].at[slot], dst_ref=self.cbuf[a].at[s, q],
            send_sem=self.send_sems.at[len(RKINDS) + q, s, a], recv_sem=self.recv_sems.at[len(RKINDS) + q, s, a],
            device_id=device(self.o, self.i, self.y, 1 - self.c), device_id_type=MESH)

    def own_copy(self, s, a, q):
        slot = slot_of(s, q // 2, q % 2, self.c)
        return pltpu.make_async_copy(self.ins[a].at[slot], self.acc[a].at[s, q], self.local.at[s, a, q])

    def hop(self, kind, s, a):
        o, i, y, c = self.o, self.i, self.y, self.c
        far, via_x, via_y, own = (self.quad(1 - i, 1 - y), self.quad(1 - i, y), self.quad(i, 1 - y), self.quad(i, y))
        acc = self.acc[a]
        plan = {
            "da": lambda: (self.half(acc.at[s, far], 0), self.far[a].at[0, s], device(o, i, 1 - y, c)),
            "db": lambda: (self.half(acc.at[s, far], 1), self.far[a].at[1, s], device(o, 1 - i, y, c)),
            "x": lambda: (acc.at[s, via_x], self.xbuf[a].at[s], device(o, 1 - i, y, c)),
            "y": lambda: (acc.at[s, via_y], self.ybuf[a].at[s], device(o, i, 1 - y, c)),
            "up": lambda: (acc.at[s, own], self.upbuf[a].at[s], device(o + 1, i, y, c)),
            "down": lambda: (acc.at[s, own], self.downbuf[a].at[s], device(o - 1, i, y, c)),
        }
        src, dst, target = plan[kind]()
        k = RKINDS.index(kind)
        return pltpu.make_async_remote_copy(
            src_ref=src, dst_ref=dst, send_sem=self.send_sems.at[k, s, a],
            recv_sem=self.recv_sems.at[k, s, a], device_id=target, device_id_type=MESH)

    def target_slice(self, t):
        return jnp.where(t % 2 == 0, self.n - 1 - t // 2, t // 2)

    def begin(self, t, carry):
        s = self.target_slice(t)
        for a in range(self.count):
            for j in range(4):
                q = 3 - j
                self.core_copy(s, a, q).start()
                self.own_copy(s, a, q).start()
        return carry

    def pair(self, s, a):
        for q in range(4):
            self.core_copy(s, a, q).wait_recv()
            self.own_copy(s, a, q).wait()
            self.acc[a][s, q] = (self.acc[a][s, q].astype(jnp.float32)
                                 + self.cbuf[a][s, q].astype(jnp.float32)).astype(jnp.bfloat16)

    def first(self, s):
        for a in range(self.count):
            self.pair(s, a)
            self.hop("da", s, a).start()
            self.hop("db", s, a).start()

    def second(self, s):
        for a in range(self.count):
            cols = self.acc[a].shape[-1] // 2
            for h, kind, q in ((0, "da", self.quad(1 - self.i, self.y)), (1, "db", self.quad(self.i, 1 - self.y))):
                self.hop(kind, s, a).wait_recv()
                window = pl.ds(h * cols, cols)
                self.acc[a][s, q, :, window] = (
                    self.acc[a][s, q, :, window].astype(jnp.float32)
                    + self.far[a][h, s].astype(jnp.float32)).astype(jnp.bfloat16)
                self.hop("x" if h == 0 else "y", s, a).start()

    def third(self, s):
        o, q = self.o, self.quad(self.i, self.y)
        for a in range(self.count):
            self.hop("x", s, a).wait_recv()
            self.hop("y", s, a).wait_recv()
            total = (self.acc[a][s, q].astype(jnp.float32) + self.xbuf[a][s].astype(jnp.float32)
                     + self.ybuf[a][s].astype(jnp.float32))

            @pl.when(s != o)
            def _():
                self.acc[a][s, q] = total.astype(jnp.bfloat16)

            @pl.when(s == o)
            def _():
                self.outs[a][...] = total

        for a in range(self.count):
            for kind, ahead, has_before, buf in (
                ("up", s > o, o > 0, self.upbuf), ("down", s < o, o < self.n - 1, self.downbuf)):

                @pl.when(ahead)
                def _(kind=kind, has_before=has_before, buf=buf, a=a):
                    @pl.when(has_before)
                    def _():
                        self.hop(kind, s, a).wait_recv()
                        self.acc[a][s, q] = (self.acc[a][s, q].astype(jnp.float32)
                                             + buf[a][s].astype(jnp.float32)).astype(jnp.bfloat16)

                    self.hop(kind, s, a).start()

    def step(self, t, carry):
        n = self.n

        @pl.when(t < n)
        def _():
            self.first(self.target_slice(t))

        @pl.when((t >= 1) & (t < n + 1))
        def _():
            self.second(self.target_slice(t - 1))

        @pl.when(t >= 2)
        def _():
            self.third(self.target_slice(t - 2))

        return carry

    def finish(self):
        o = self.o
        for a in range(self.count):
            for kind, there, buf in (("up", o > 0, self.upbuf), ("down", o < self.n - 1, self.downbuf)):

                @pl.when(there)
                def _(kind=kind, buf=buf, a=a):
                    self.hop(kind, o, a).wait_recv()
                    self.outs[a][...] += buf[a][o].astype(jnp.float32)

        def close(s, carry):
            for a in range(self.count):
                for q in range(4):
                    self.core_copy(s, a, q).wait_send()
                for kind in ("da", "db", "x", "y"):
                    self.hop(kind, s, a).wait_send()

                @pl.when(s > o)
                def _(a=a):
                    self.hop("up", s, a).wait_send()

                @pl.when(s < o)
                def _(a=a):
                    self.hop("down", s, a).wait_send()

            return carry

        lax.fori_loop(0, self.n, close, 0)

    def run(self):
        lax.fori_loop(0, self.n, self.begin, 0)
        lax.fori_loop(0, self.n + 2, self.step, 0)
        self.finish()


def scatter_scratch(n, shapes):
    bf = jnp.bfloat16
    scratch = [pltpu.VMEM((n, 4) + s, bf) for s in shapes]
    scratch += [pltpu.VMEM((n, 4) + s, bf) for s in shapes]
    scratch += [pltpu.VMEM((2, n, s[0], s[1] // 2), bf) for s in shapes]
    for _ in range(4):
        scratch += [pltpu.VMEM((n,) + s, bf) for s in shapes]
    count = len(shapes)
    scratch += [pltpu.SemaphoreType.DMA((len(RKINDS) + 4, n, count)) for _ in range(2)]
    scratch += [pltpu.SemaphoreType.DMA((n, count, 4))]
    return scratch


def scatter_rows(blocks, collective_id):
    n_outer = lax.axis_size("dp") // 2
    count = len(blocks)
    shapes = [b.shape[1:] for b in blocks]

    def kernel(*refs):
        ins, outs, scratch = refs[:count], refs[count:2 * count], refs[2 * count:]
        work = Scatter(n_outer, ins, outs, scratch)
        greet(n_outer, *placement())
        work.run()

    return pl.pallas_call(
        kernel,
        out_shape=[jax.ShapeDtypeStruct(s, jnp.float32) for s in shapes],
        in_specs=[pl.BlockSpec(memory_space=pl.ANY)] * count,
        out_specs=[pl.BlockSpec(memory_space=pltpu.VMEM)] * count,
        scratch_shapes=scatter_scratch(n_outer, shapes),
        compiler_params=pltpu.CompilerParams(collective_id=collective_id, has_side_effects=True, vmem_limit_bytes=56 << 20),
        name="scatter_rows",
    )(*blocks)


def norm_rows(values):
    centred = values - jnp.mean(values, axis=-1, keepdims=True)
    spread = jnp.mean(centred * centred, axis=-1, keepdims=True)
    inverse = lax.rsqrt(spread + 1e-05)
    return (centred * inverse, inverse)


def norm_back(grad_in, normed, inverse):
    mean_grad = jnp.mean(grad_in, axis=-1, keepdims=True)
    mean_prod = jnp.mean(grad_in * normed, axis=-1, keepdims=True)
    return (grad_in - mean_grad - normed * mean_prod) * inverse


def swap_halves(values):
    lane = lax.broadcasted_iota(jnp.int32, values.shape, 1)
    half = HEAD_DIM // 2
    return jnp.where(
        lane % HEAD_DIM < half, pltpu.roll(values, 128 - half, 1), pltpu.roll(values, half, 1)
    )


def rope_tables(positions):
    exponent = jnp.arange(HEAD_DIM // 2, dtype=jnp.float32) * (2.0 / HEAD_DIM)
    frequency = 10000.0 ** (-exponent)
    angles = positions.astype(jnp.float32)[:, None] * frequency[None, :]
    cosine, sine = jnp.cos(angles), jnp.sin(angles)
    return jnp.concatenate([cosine] * 4, -1), jnp.concatenate([-sine, sine, -sine, sine], -1)


def project_kernel(slots, scale, n_ref, w_ref, cos_ref, sin_ref, q_ref, kv_ref):
    j = pl.program_id(0)
    cosine, sine = cos_ref[...], sin_ref[...]
    local = cosine.shape[0]
    for s in range(slots):
        rows = pl.ds(s * local, local)
        part = jnp.dot(n_ref[rows, :], w_ref[...], preferred_element_type=jnp.float32)
        for g in range(part.shape[1] // 128):
            cols = pl.ds(g * 128, 128)
            piece = part[:, g * 128:(g + 1) * 128]

            @pl.when(j < 2)
            def _():
                turned = (piece * cosine + swap_halves(piece) * sine).astype(jnp.bfloat16)
                q_ref[rows, cols] = (turned.astype(jnp.float32) * scale).astype(jnp.bfloat16)

            @pl.when((j >= 2) & (j < 4))
            def _():
                kv_ref[rows, cols] = (piece * cosine + swap_halves(piece) * sine).astype(jnp.bfloat16)

            @pl.when(j >= 4)
            def _():
                kv_ref[rows, cols] = piece.astype(jnp.bfloat16)


def project_rows(normed, weight, cosine, sine, slots):
    rows, width = normed.shape
    tile = width // 2
    return pl.pallas_call(
        functools.partial(project_kernel, slots, HEAD_DIM ** -0.5),
        grid=(6,),
        out_shape=[jax.ShapeDtypeStruct((rows, width), jnp.bfloat16),
                   jax.ShapeDtypeStruct((rows, 2 * width), jnp.bfloat16)],
        in_specs=[pl.BlockSpec((rows, width), lambda j: (0, 0)),
                  pl.BlockSpec((width, tile), lambda j: (0, j)),
                  pl.BlockSpec(cosine.shape, lambda j: (0, 0)),
                  pl.BlockSpec(sine.shape, lambda j: (0, 0))],
        out_specs=[pl.BlockSpec((rows, tile), lambda j: (0, jnp.minimum(j, 1))),
                   pl.BlockSpec((rows, tile), lambda j: (0, jnp.maximum(j - 2, 0)))],
        compiler_params=pltpu.CompilerParams(vmem_limit_bytes=40 << 20),
        name="project_rows",
    )(normed, weight, cosine, sine)


def chip_greet(o, i, y, c):
    barrier = pltpu.get_barrier_semaphore()
    for target in (device(o, i, 1 - y, c), device(o, i, y, 1 - c)):
        pl.semaphore_signal(barrier, inc=1, device_id=target, device_id_type=MESH)
    pl.semaphore_wait(barrier, 2)


def share_kernel(slots, own_ref, all_ref, send, recv, local):
    o, i, y, c = placement()
    chip_greet(o, i, y, c)
    mate, across = device(o, i, y, 1 - c), device(o, i, 1, c)
    mine = y * 2 + c

    def hop(kind, s, src, piece, target):
        return pltpu.make_async_remote_copy(
            src_ref=src, dst_ref=all_ref.at[piece, s], send_sem=send.at[kind, s],
            recv_sem=recv.at[kind, s], device_id=target, device_id_type=MESH)

    for s in range(slots):
        @pl.when(y == 0)
        def _(s=s):
            hop(0, s, own_ref.at[s], mine, across).start()

        hop(1, s, own_ref.at[s], mine, mate).start()
        pltpu.make_async_copy(own_ref.at[s], all_ref.at[mine, s], local.at[s]).start()
    for s in range(slots):
        @pl.when(y == 1)
        def _(s=s):
            hop(0, s, own_ref.at[s], c, mate).wait_recv()
            hop(2, s, all_ref.at[c, s], c, mate).start()
    for s in range(slots):
        hop(1, s, own_ref.at[s], y * 2 + 1 - c, mate).wait_recv()
        hop(1, s, own_ref.at[s], mine, mate).wait_send()
        pltpu.make_async_copy(own_ref.at[s], all_ref.at[mine, s], local.at[s]).wait()

        @pl.when(y == 0)
        def _(s=s):
            hop(0, s, own_ref.at[s], mine, across).wait_send()

        @pl.when(y == 1)
        def _(s=s):
            hop(2, s, all_ref.at[1 - c, s], 1 - c, mate).wait_recv()
            hop(2, s, all_ref.at[c, s], c, mate).wait_send()


def share_keys(own, collective_id):
    slots = own.shape[0]
    return pl.pallas_call(
        functools.partial(share_kernel, slots),
        out_shape=jax.ShapeDtypeStruct((4,) + own.shape, own.dtype),
        in_specs=[pl.BlockSpec(memory_space=pl.ANY)],
        out_specs=pl.BlockSpec(memory_space=pl.ANY),
        scratch_shapes=[pltpu.SemaphoreType.DMA((3, slots)), pltpu.SemaphoreType.DMA((3, slots)),
                        pltpu.SemaphoreType.DMA((slots,))],
        compiler_params=pltpu.CompilerParams(collective_id=collective_id, has_side_effects=True),
        name="share_keys",
    )(own)


def collect_kernel(slots, width, dk_ref, dv_ref, cos_ref, sin_ref, out_ref,
                   own, mate_buf, far_mine, far_mate, far_sum, far_buf, send, recv, local):
    o, i, y, c = placement()
    chip_greet(o, i, y, c)
    mate, across = device(o, i, y, 1 - c), device(o, i, 0, c)
    mine, other = y * 2 + c, y * 2 + 1 - c
    parts = (dk_ref, dv_ref)

    def hop(kind, s, p, src, dst, target):
        return pltpu.make_async_remote_copy(
            src_ref=src, dst_ref=dst, send_sem=send.at[kind, s, p], recv_sem=recv.at[kind, s, p],
            device_id=target, device_id_type=MESH)

    def near(s, p):
        return hop(0, s, p, parts[p].at[other, s], mate_buf.at[s, p], mate)

    def far(s, p):
        return hop(1, s, p, parts[p].at[1 - c, s], far_mate.at[s, p], mate)

    def back(s, p):
        return hop(2, s, p, far_sum.at[s, p], far_buf.at[s, p], across)

    def load(s, p):
        return pltpu.make_async_copy(parts[p].at[mine, s], own.at[s, p], local.at[0, s, p])

    def load_far(s, p):
        return pltpu.make_async_copy(parts[p].at[c, s], far_mine.at[s, p], local.at[1, s, p])

    every = [(s, p) for s in range(slots) for p in range(2)]
    for s, p in every:
        @pl.when(y == 1)
        def _(s=s, p=p):
            far(s, p).start()
            load_far(s, p).start()

        near(s, p).start()
        load(s, p).start()
    for s, p in every:
        @pl.when(y == 1)
        def _(s=s, p=p):
            far(s, p).wait_recv()
            load_far(s, p).wait()
            far_sum[s, p] = (far_mine[s, p].astype(jnp.float32)
                             + far_mate[s, p].astype(jnp.float32)).astype(jnp.bfloat16)
            back(s, p).start()

    cosine, sine = cos_ref[...], sin_ref[...]

    def put(s, p, total):
        for g in range(width // 128):
            cols = slice(g * 128, (g + 1) * 128)
            piece = total[:, cols]
            if p == 0:
                piece = piece * cosine - swap_halves(piece) * sine
            out_ref[s, :, pl.ds(p * width + g * 128, 128)] = piece.astype(jnp.bfloat16)

    for s, p in every:
        near(s, p).wait_recv()
        load(s, p).wait()

        @pl.when(y == 0)
        def _(s=s, p=p):
            back(s, p).wait_recv()
            put(s, p, own[s, p].astype(jnp.float32) + mate_buf[s, p].astype(jnp.float32)
                + far_buf[s, p].astype(jnp.float32))

        @pl.when(y == 1)
        def _(s=s, p=p):
            put(s, p, own[s, p].astype(jnp.float32) + mate_buf[s, p].astype(jnp.float32))

    for s, p in every:
        near(s, p).wait_send()

        @pl.when(y == 1)
        def _(s=s, p=p):
            far(s, p).wait_send()
            back(s, p).wait_send()


def collect_keys(dk, dv, cosine, sine, collective_id):
    _, slots, local, width = dk.shape
    buffer = pltpu.VMEM((slots, 2, local, width), jnp.bfloat16)
    return pl.pallas_call(
        functools.partial(collect_kernel, slots, width),
        out_shape=jax.ShapeDtypeStruct((slots, local, 2 * width), jnp.bfloat16),
        in_specs=[pl.BlockSpec(memory_space=pl.ANY)] * 2 + [pl.BlockSpec(memory_space=pltpu.VMEM)] * 2,
        out_specs=pl.BlockSpec(memory_space=pltpu.VMEM),
        scratch_shapes=[buffer] * 6 + [pltpu.SemaphoreType.DMA((3, slots, 2))] * 2
        + [pltpu.SemaphoreType.DMA((2, slots, 2))],
        compiler_params=pltpu.CompilerParams(collective_id=collective_id, has_side_effects=True, vmem_limit_bytes=40 << 20),
        name="collect_keys",
    )(dk, dv, cosine, sine)


def masked_scores(query, keys, offset, length):
    scores = lax.dot_general(query, keys, (((1,), (1,)), ((), ())), preferred_element_type=jnp.float32)
    rows = lax.broadcasted_iota(jnp.int32, scores.shape, 0) + offset
    cols = lax.broadcasted_iota(jnp.int32, scores.shape, 1)
    return jnp.where((cols <= rows) & (cols < length), scores, -1e30)


def one_head(values, h):
    lane = lax.broadcasted_iota(jnp.int32, values.shape, 1)
    keep = (lane < HEAD_DIM) if h == 0 else (lane >= HEAD_DIM)
    return jnp.where(keep, values, jnp.zeros_like(values))


def join_heads(first, second):
    lane = lax.broadcasted_iota(jnp.int32, first.shape, 1)
    return jnp.where(lane < HEAD_DIM, first, second)


def forward_kernel(pieces, lens_ref, seq_ref, q_ref, k_ref, v_ref, o_ref, log_ref):
    s = pl.program_id(0)
    local = q_ref.shape[1]
    length, seq = lens_ref[s], seq_ref[0]
    live = seq * local < length

    @pl.when(jnp.logical_not(live))
    def _():
        o_ref[...] = jnp.zeros_like(o_ref)
        log_ref[...] = jnp.zeros_like(log_ref)

    for n in range(1, pieces + 1):
        @pl.when(live & (seq == n - 1))
        def _(n=n):
            query = q_ref[0]
            keys = k_ref[:n, 0].reshape(n * local, 128)
            values = v_ref[:n, 0].reshape(n * local, 128)
            mixed, logs = [], []
            for h in range(2):
                scores = masked_scores(one_head(query, h), keys, (n - 1) * local, length)
                top = jnp.max(scores, axis=1, keepdims=True)
                terms = jnp.exp(scores - top)
                total = jnp.sum(terms, axis=1, keepdims=True)
                mix = jnp.dot(terms.astype(jnp.bfloat16), values, preferred_element_type=jnp.float32)
                mixed.append(mix / total)
                logs.append(jnp.broadcast_to(top + jnp.log(total), (local, 128)))
            o_ref[0] = join_heads(*mixed).astype(jnp.bfloat16)
            log_ref[0] = join_heads(*logs)


def backward_kernel(pieces, scale, lens_ref, seq_ref, q_ref, k_ref, v_ref, do_ref, log_ref, cos_ref, sin_ref,
                    dq_ref, dk_ref, dv_ref):
    s = pl.program_id(0)
    local = q_ref.shape[1]
    length, seq = lens_ref[s], seq_ref[0]
    live = seq * local < length

    @pl.when(jnp.logical_not(live))
    def _():
        dq_ref[...] = jnp.zeros_like(dq_ref)
        dk_ref[...] = jnp.zeros_like(dk_ref)
        dv_ref[...] = jnp.zeros_like(dv_ref)

    def across(left, right):
        return lax.dot_general(left, right, (((0,), (0,)), ((), ())), preferred_element_type=jnp.float32)

    for n in range(1, pieces + 1):
        @pl.when(live & (seq == n - 1))
        def _(n=n):
            query, grad = q_ref[0], do_ref[0]
            keys = k_ref[:n, 0].reshape(n * local, 128)
            values = v_ref[:n, 0].reshape(n * local, 128)
            dq, dk, dv = [], [], []
            for h in range(2):
                scores = masked_scores(one_head(query, h), keys, (n - 1) * local, length)
                probs = jnp.exp(scores - log_ref[0, :, h * HEAD_DIM:h * HEAD_DIM + 1])
                dprobs = lax.dot_general(one_head(grad, h), values, (((1,), (1,)), ((), ())),
                                         preferred_element_type=jnp.float32)
                inner = jnp.sum(probs * dprobs, axis=1, keepdims=True)
                dscores = (probs * (dprobs - inner)).astype(jnp.bfloat16)
                dq.append(jnp.dot(dscores, keys, preferred_element_type=jnp.float32))
                dk.append(across(dscores, query))
                dv.append(across(probs.astype(jnp.bfloat16), grad))
            turn = join_heads(*dq) * scale
            dq_ref[0] = (turn * cos_ref[...] - swap_halves(turn) * sin_ref[...]).astype(jnp.bfloat16)
            dk_ref[:n, 0] = join_heads(*dk).astype(jnp.bfloat16).reshape(n, local, 128)
            dv_ref[:n, 0] = join_heads(*dv).astype(jnp.bfloat16).reshape(n, local, 128)
            if n < pieces:
                rest = jnp.zeros((pieces - n, local, 128), jnp.bfloat16)
                dk_ref[n:, 0] = rest
                dv_ref[n:, 0] = rest


def attend_specs(pieces, local, pairs):
    row = pl.BlockSpec((1, local, 128), lambda s, h, *_: (s, 0, h))
    key = pl.BlockSpec((pieces, 1, local, 128), lambda s, h, *_: (0, s, 0, h))
    value = pl.BlockSpec((pieces, 1, local, 128), lambda s, h, *_: (0, s, 0, h + pairs))
    return row, key, value


def attend(query, kv_all, lengths):
    slots, local, width = query.shape
    pieces, pairs = kv_all.shape[0], width // 128
    row, key, value = attend_specs(pieces, local, pairs)
    seq = lax.axis_index("seq").astype(jnp.int32)[None]
    return pl.pallas_call(
        functools.partial(forward_kernel, pieces),
        grid_spec=pltpu.PrefetchScalarGridSpec(
            num_scalar_prefetch=2, grid=(slots, pairs), in_specs=[row, key, value], out_specs=[row, row]),
        out_shape=[jax.ShapeDtypeStruct(query.shape, jnp.bfloat16), jax.ShapeDtypeStruct(query.shape, jnp.float32)],
        compiler_params=pltpu.CompilerParams(vmem_limit_bytes=40 << 20),
        name="attend",
    )(lengths, seq, query, kv_all, kv_all)


def attend_back(query, kv_all, grad, log_total, lengths, cosine, sine):
    slots, local, width = query.shape
    pieces, pairs = kv_all.shape[0], width // 128
    row, key, value = attend_specs(pieces, local, pairs)
    table = pl.BlockSpec(cosine.shape, lambda s, h, *_: (0, 0))
    seq = lax.axis_index("seq").astype(jnp.int32)[None]
    shared = jax.ShapeDtypeStruct((pieces, slots, local, width), jnp.bfloat16)
    return pl.pallas_call(
        functools.partial(backward_kernel, pieces, HEAD_DIM ** -0.5),
        grid_spec=pltpu.PrefetchScalarGridSpec(
            num_scalar_prefetch=2, grid=(slots, pairs),
            in_specs=[row, key, value, row, row, table, table], out_specs=[row, key, key]),
        out_shape=[jax.ShapeDtypeStruct(query.shape, jnp.bfloat16), shared, shared],
        compiler_params=pltpu.CompilerParams(vmem_limit_bytes=48 << 20),
        name="attend_back",
    )(lengths, seq, query, kv_all, kv_all, grad, log_total, cosine, sine)


def contract_last(left_side, right_side):
    return lax.dot_general(
        left_side, right_side, (((1,), (1,)), ((), ())), preferred_element_type=jnp.float32
    )


def gather_weights(first, second, collective_id):
    one, two = gather_rows((first, second), collective_id)
    return one.reshape(-1, first.shape[1]), two.reshape(-1, second.shape[1])


def weight_term(left_side, right_side):
    term = lax.dot_general(
        left_side, right_side, (((0,), (0,)), ((), ())), preferred_element_type=jnp.float32
    )
    return term.astype(jnp.bfloat16).reshape(lax.axis_size(("dp", "seq")), -1, term.shape[1])


def on_device(tokens, lengths, w_qkv, w_att_out, w_ffin, w_ffout, cotangent):
    slot_count, local_len, model_width = tokens.shape
    row_count = slot_count * local_len
    positions = lax.axis_index("seq") * local_len + jnp.arange(local_len, dtype=jnp.int32)
    valid_rows = (positions[None, :] < lengths[:, None]).astype(jnp.float32)[:, :, None]
    cosine, sine_table = rope_tables(positions)
    inputs = tokens.astype(jnp.float32).reshape(row_count, model_width)
    normed_one, inverse_one = norm_rows(inputs)
    normed_one_bf = normed_one.astype(jnp.bfloat16)
    qkv_full, att_out_full = gather_weights(w_qkv, w_att_out, 1)
    query_rows, kv_rows = project_rows(normed_one_bf, qkv_full, cosine, sine_table, slot_count)
    query_bf = query_rows.reshape(tokens.shape)
    kv_all = share_keys(kv_rows.reshape(slot_count, local_len, 2 * model_width), 4)
    mixed_slots, log_total = attend(query_bf, kv_all, lengths)
    mixed_bf = mixed_slots.reshape(row_count, model_width)
    hidden_state = inputs + jnp.dot(mixed_bf, att_out_full, preferred_element_type=jnp.float32)
    normed_two, inverse_two = norm_rows(hidden_state)
    normed_two_bf = normed_two.astype(jnp.bfloat16)
    ffin_full, ffout_full = gather_weights(w_ffin, w_ffout, 2)
    gate_up = jnp.dot(normed_two_bf, ffin_full, preferred_element_type=jnp.float32)
    half_units = gate_up.shape[1] // 2
    up_part = gate_up[:, :half_units]
    gate_part = gate_up[:, half_units:]
    gate_sigmoid = jax.nn.sigmoid(gate_part)
    activated_bf = (gate_part * gate_sigmoid * up_part).astype(jnp.bfloat16)
    branch = jnp.dot(activated_bf, ffout_full, preferred_element_type=jnp.float32)
    block_output = (valid_rows * (hidden_state + branch).reshape(tokens.shape)).astype(jnp.bfloat16)
    grad_out = (valid_rows * cotangent.astype(jnp.float32)).reshape(row_count, model_width)
    grad_out_bf = grad_out.astype(jnp.bfloat16)
    ffin_back, ffout_back = ffin_full, ffout_full
    grad_act = contract_last(grad_out_bf, ffout_back)
    grad_up = grad_act * gate_part * gate_sigmoid
    grad_gate = grad_act * up_part * gate_sigmoid * (1.0 + gate_part * (1.0 - gate_sigmoid))
    grad_gate_up_bf = jnp.concatenate([grad_up, grad_gate], 1).astype(jnp.bfloat16)
    grad_normed_two = contract_last(grad_gate_up_bf, ffin_back)
    grad_hidden = grad_out + norm_back(grad_normed_two, normed_two, inverse_two)
    grad_hidden_bf = grad_hidden.astype(jnp.bfloat16)
    qkv_back, att_out_back = qkv_full, att_out_full
    grad_mixed_bf = contract_last(grad_hidden_bf, att_out_back).astype(jnp.bfloat16)
    grad_query, grad_key_all, grad_value_all = attend_back(
        query_bf, kv_all, grad_mixed_bf.reshape(tokens.shape), log_total, lengths, cosine, sine_table
    )
    grad_kv = collect_keys(grad_key_all, grad_value_all, cosine, sine_table, 5)
    grad_project_bf = jnp.concatenate([grad_query, grad_kv], 2).reshape(row_count, 3 * model_width)
    grad_normed_one = contract_last(grad_project_bf, qkv_back)
    grad_tokens = grad_hidden + norm_back(grad_normed_one, normed_one, inverse_one)
    grad_qkv, grad_att_out, grad_ffin, grad_ffout = scatter_rows(
        (
            weight_term(normed_one_bf, grad_project_bf),
            weight_term(mixed_bf, grad_hidden_bf),
            weight_term(normed_two_bf, grad_gate_up_bf),
            weight_term(activated_bf, grad_out_bf),
        ),
        3,
    )
    return (
        block_output,
        grad_tokens.reshape(tokens.shape),
        grad_qkv,
        grad_att_out,
        grad_ffin,
        grad_ffout,
    )


def solution(mesh):
    placed = (
        P("dp", "seq", None),
        P("dp"),
        P(("dp", "seq"), None),
        P(("dp", "seq"), None),
        P(("dp", "seq"), None),
        P(("dp", "seq"), None),
        P("dp", "seq", None),
    )
    return jax.shard_map(
        on_device,
        mesh=mesh,
        in_specs=placed,
        out_specs=(
            P("dp", "seq", None),
            P("dp", "seq", None),
            P(("dp", "seq"), None),
            P(("dp", "seq"), None),
            P(("dp", "seq"), None),
            P(("dp", "seq"), None),
        ),
        check_vma=False,
    )
```
